32 devices in a mesh: head: 4 (over z), outer: 4 (over x, core), inner: 2 (over y).
Axes of the slice: x: 2, y: 2, z: 4, core: 2. Of those that a mesh axis runs over, the one named last changes fastest.
Arguments:
- query_nope: bfloat16 [1024, 2048], P(('outer', 'inner'), 'head'), may hold values from -6 to 6
- query_rope: bfloat16 [1024, 1024], P(('outer', 'inner'), 'head'), may hold values from -8 to 8
- cache: bfloat16 [1024, 576], P(('outer', 'inner')), may hold values from -8 to 8
- span_ids: int32 [16], P(('outer', 'inner')), may hold values from 0 to 15, as said below
- key_up: bfloat16 [512, 2048], P(None, 'head'), may hold values from -0.25 to 0.25
- value_up: bfloat16 [512, 2048], P(None, 'head'), may hold values from -1.5 to 1.5
- out_proj: bfloat16 [2048, 2048], P('head'), may hold values from -1.1953125 to 1.1953125
Outputs:
- mixed: bfloat16 [1024, 2048], P(('outer', 'inner'), 'head')
The draws below stay inside these ranges and needn't reach their ends.
Inputs may be any that keep to these rules, and one draw needn't show every extreme that they name: `span_ids`: each of 0 to 15 appears once; entries 2 r and 2 r + 1 belong to storage rows r * 128 to (r + 1) * 128 - 1.
All inputs are finite; a program needn't handle non-finite values.
Results may differ from the reference program's by a relative error of at most 0.014.
Values may be sent and summed in bfloat16 or wider, within the bound.
A program may use at most 64 MiB of HBM per device.

```python
import math
import jax
import jax.numpy as jnp
from jax import lax

HEADS = 16
LATENT = 512
ROPE = 64
NOPE = 128
VDIM = 128
MODEL = 2048
SPAN = 64
SPANS = 16
SEQ = 1024


def span_order(key):
    return jax.random.permutation(jax.random.fold_in(key, 7), SPANS).astype(jnp.int32)


def draw_span_ids(key, part):
    return span_order(key)


def draw_cache(key, part):
    values_all = jax.random.normal(jax.random.fold_in(key, 1), (SEQ, LATENT + ROPE), jnp.float32)
    return jnp.clip(values_all, -8.0, 8.0).astype(jnp.bfloat16)


def draw_query_rope(key, part):
    values_all = jax.random.normal(jax.random.fold_in(key, 3), (SEQ, HEADS * ROPE), jnp.float32)
    return jnp.clip(values_all, -8.0, 8.0).astype(jnp.bfloat16)


def block_levels(rng, shape, split, least, high):
    level, own = 1.0, jax.random.fold_in(rng, 6)
    for dim, blocks in split:
        draws = jnp.exp(jax.random.uniform(jax.random.fold_in(own, dim), (blocks,), jnp.float32, least / len(split), high / len(split)))
        level = level * jnp.repeat(draws, shape[dim] // blocks).reshape([-1 if axis == dim else 1 for axis in range(len(shape))])
    return level


def scatter_about(stream_key, shape, width, reach, pieces=(), kind=jnp.bfloat16):
    drawn = width * jax.random.normal(stream_key, shape, jnp.float32)
    if pieces:
        drawn = drawn * block_levels(stream_key, shape, pieces, -0.22, 0.18)
    return jnp.clip(drawn, -reach, reach).astype(kind)


def setup_inputs(seed: int = 0) -> dict:
    key_of = jax.random.split(jax.random.key(seed), 8)
    return {
        "query_nope": scatter_about(key_of[0], (SEQ, HEADS * NOPE), 1.0, 6.0, ((0, 8), (1, 4))),
        "query_rope": draw_query_rope(jax.random.fold_in(key_of[7], 71), 0),
        "cache": draw_cache(jax.random.fold_in(key_of[7], 71), 0),
        "span_ids": draw_span_ids(jax.random.fold_in(key_of[7], 71), 0),
        "key_up": scatter_about(key_of[4], (LATENT, HEADS * NOPE), LATENT ** -0.5, 0.25, ((1, 4),)),
        "value_up": scatter_about(key_of[5], (LATENT, HEADS * VDIM), 0.25, 1.5, ((1, 4),)),
        "out_proj": scatter_about(key_of[6], (HEADS * VDIM, MODEL), 0.2, 1.1953125, ((0, 4),)),
    }


def reference(query_nope, query_rope, cache, span_ids, key_up, value_up, out_proj):
    seq_total = cache.shape[0]
    row_ids = jnp.arange(seq_total, dtype=jnp.int32)
    position = span_ids[row_ids // SPAN] * SPAN + row_ids % SPAN
    query_heads = query_nope.reshape(seq_total, HEADS, NOPE).astype(jnp.float32)
    key_weight = key_up.reshape(LATENT, HEADS, NOPE).astype(jnp.float32)
    q_latent = jnp.einsum("shd,chd->hsc", query_heads, key_weight).astype(jnp.bfloat16)
    q_rotary = jnp.transpose(query_rope.reshape(seq_total, HEADS, ROPE), (1, 0, 2))
    queries = jnp.concatenate([q_latent, q_rotary], axis=2).astype(jnp.float32)
    keys_all = cache.astype(jnp.float32)
    latent_all = keys_all[:, :LATENT]
    value_weight = value_up.reshape(LATENT, HEADS, VDIM).astype(jnp.float32)
    softmax_scale = (NOPE + ROPE) ** -0.5
    block_rows = math.gcd(seq_total, 512)

    def one_block(which_block):
        first_row = which_block * block_rows
        query_block = lax.dynamic_slice_in_dim(queries, first_row, block_rows, 1)
        query_pos = lax.dynamic_slice_in_dim(position, first_row, block_rows, 0)
        scores = jnp.einsum("hsc,tc->hst", query_block, keys_all) * softmax_scale
        visible = position[None, None, :] <= query_pos[None, :, None]
        scores = jnp.where(visible, scores, -jnp.inf)
        row_max = jnp.max(scores, axis=2, keepdims=True)
        expsum = jnp.exp(scores - row_max)
        denom = jnp.sum(expsum, axis=2)
        weights = lax.optimization_barrier(expsum.astype(jnp.bfloat16)).astype(jnp.float32)
        latent_out = jnp.einsum("hst,tc->hsc", weights, latent_all) / denom[:, :, None]
        latent_out = lax.optimization_barrier(latent_out.astype(jnp.bfloat16)).astype(jnp.float32)
        head_out = jnp.einsum("hsc,chd->shd", latent_out, value_weight)
        head_out = head_out.astype(jnp.bfloat16).reshape(block_rows, HEADS * VDIM)
        mixed = jnp.dot(head_out, out_proj, preferred_element_type=jnp.float32)
        return mixed.astype(jnp.bfloat16)

    blocks = lax.map(one_block, jnp.arange(seq_total // block_rows, dtype=jnp.int32))
    return blocks.reshape(seq_total, MODEL)
```

```python
import functools
import math

import jax
import jax.numpy as jnp
from jax import lax
from jax.experimental import pallas as pl
from jax.experimental.pallas import tpu as pltpu
from jax.sharding import PartitionSpec as P

LATENT = 512
ROPE = 64
NOPE = 128
VDIM = 128
SPAN = 64
CORES = 2
MESH = pl.DeviceIdType.MESH


def loop(start, stop, body):
    if stop - start <= 4:
        for step in range(start, stop):
            body(step)
    else:
        lax.fori_loop(start, stop, lambda step, carry: (body(step), carry)[1], 0)


def kernel(
    sizes,
    nope_hbm,
    rope_hbm,
    cache_hbm,
    kpos_hbm,
    qpos_hbm,
    key_up_hbm,
    value_up_hbm,
    out_proj_hbm,
    mixed_ref,
    nope,
    rope,
    kv,
    kpos,
    qpos,
    key_up,
    value_up,
    out_proj,
    queries,
    acc,
    top,
    total,
    head_out,
    outbox,
    inbox,
    local_sem,
    send_sem,
    recv_sem,
    fsend_sem,
    frecv_sem,
    zsend_sem,
    zrecv_sem,
):
    n_head, n_outer, n_inner = sizes
    chip_rows = n_outer // CORES
    chips = chip_rows * n_inner
    rows = cache_hbm.shape[0]
    heads = key_up_hbm.shape[1] // NOPE
    cols = mixed_ref.shape[1]
    head = lax.axis_index("head")
    outer = lax.axis_index("outer")
    inner = lax.axis_index("inner")
    core = lax.rem(outer, CORES)
    chip_row = outer // CORES
    peer = {"outer": chip_row * CORES + 1 - core}

    def chip(r):
        to_row = lax.rem(chip_row + r // n_inner, chip_rows)
        to_col = lax.rem(inner + r % n_inner, n_inner)
        return {"outer": to_row * CORES + core, "inner": to_col}

    def head_dev(k):
        return {"head": lax.rem(head + k, n_head)}

    mine, other = pl.ds(0, rows), pl.ds(rows, rows)
    loads = [
        pltpu.make_async_copy(src, dst, local_sem.at[slot])
        for slot, (src, dst) in enumerate(
            (
                (cache_hbm, kv.at[0, mine]),
                (kpos_hbm, kpos.at[0, 0]),
                (nope_hbm, nope),
                (key_up_hbm, key_up),
                (rope_hbm, rope),
                (qpos_hbm, qpos),
                (value_up_hbm, value_up),
                (out_proj_hbm, out_proj),
            )
        )
    ]
    for load in loads:
        load.start()

    barrier = pltpu.get_barrier_semaphore()
    pl.semaphore_signal(barrier, inc=1, device_id=peer, device_id_type=MESH)
    loop(
        1,
        chips,
        lambda r: pl.semaphore_signal(barrier, inc=1, device_id=chip(r), device_id_type=MESH),
    )
    loop(
        1,
        n_head,
        lambda k: pl.semaphore_signal(barrier, inc=1, device_id=head_dev(k), device_id_type=MESH),
    )
    pl.semaphore_wait(barrier, 1 + (chips - 1) + (n_head - 1))

    def sends(r):
        return (
            pltpu.make_async_remote_copy(
                src_ref=kv.at[0, mine],
                dst_ref=kv.at[r, mine],
                send_sem=send_sem.at[0, r],
                recv_sem=recv_sem.at[0, r],
                device_id=chip(r),
                device_id_type=MESH,
            ),
            pltpu.make_async_remote_copy(
                src_ref=kpos.at[0, 0],
                dst_ref=kpos.at[r, 0],
                send_sem=send_sem.at[1, r],
                recv_sem=recv_sem.at[1, r],
                device_id=chip(r),
                device_id_type=MESH,
            ),
        )

    def forwards(r):
        return (
            pltpu.make_async_remote_copy(
                src_ref=kv.at[r, mine],
                dst_ref=kv.at[r, other],
                send_sem=fsend_sem.at[0, r],
                recv_sem=frecv_sem.at[0, r],
                device_id=peer,
                device_id_type=MESH,
            ),
            pltpu.make_async_remote_copy(
                src_ref=kpos.at[r, 0],
                dst_ref=kpos.at[r, 1],
                send_sem=fsend_sem.at[1, r],
                recv_sem=frecv_sem.at[1, r],
                device_id=peer,
                device_id_type=MESH,
            ),
        )

    def start_all(copies):
        for copy in copies:
            copy.start()

    loads[0].wait()
    loads[1].wait()
    loop(1, chips, lambda r: start_all(sends(r)))
    start_all(forwards(0))

    loads[2].wait()
    loads[3].wait()
    loads[4].wait()
    for h in range(heads):
        block = slice(h * NOPE, (h + 1) * NOPE)
        q_latent = lax.dot_general(
            nope[:, block],
            key_up[:, block],
            (((1,), (1,)), ((), ())),
            preferred_element_type=jnp.float32,
        )
        queries[h * rows : (h + 1) * rows, :LATENT] = q_latent.astype(jnp.bfloat16)
        queries[h * rows : (h + 1) * rows, LATENT:] = rope[:, h * ROPE : (h + 1) * ROPE]
    loads[5].wait()

    scale = (NOPE + ROPE) ** (-0.5) * math.log2(math.e)

    def attend(r, first):
        for copy in forwards(r):
            copy.wait_recv()
        keys = kv[r]
        scores = (
            lax.dot_general(
                queries[...], keys, (((1,), (1,)), ((), ())), preferred_element_type=jnp.float32
            )
            * scale
        )
        at_key = jnp.concatenate([kpos[r, 0][:1], kpos[r, 1][:1]], axis=1)
        at_query = qpos[:, :1]
        visible = at_key <= at_query
        scores = jnp.where(
            visible[None], scores.reshape(heads, rows, CORES * rows), -jnp.inf
        ).reshape(heads * rows, CORES * rows)
        high = jnp.max(scores, axis=1, keepdims=True)
        if not first:
            before = top[...]
            high = jnp.maximum(before, high)
            rescale = jnp.exp2(before - high)
        weights = jnp.exp2(scores - high)
        added = jnp.sum(weights, axis=1, keepdims=True)
        part = jnp.dot(
            weights.astype(jnp.bfloat16), keys[:, :LATENT], preferred_element_type=jnp.float32
        )
        top[...] = high
        if first:
            total[...] = added
            acc[...] = part
        else:
            total[...] = total[...] * rescale + added
            acc[...] = acc[...] * rescale + part

    def relay(r):
        for copy in sends(r):
            copy.wait_recv()
        start_all(forwards(r))

    attend(0, True)
    if chips <= 4:
        for r in range(1, min(chips, 3)):
            relay(r)
        for r in range(1, min(chips, 3)):
            attend(r, False)
        for r in range(3, chips):
            relay(r)
            attend(r, False)
    else:
        loop(1, chips, relay)
        loop(1, chips, lambda r: attend(r, False))

    loads[6].wait()
    loads[7].wait()
    for h in range(heads):
        block = slice(h * rows, (h + 1) * rows)
        latent_out = (acc[block] / total[block]).astype(jnp.bfloat16)
        head_out[:, h * VDIM : (h + 1) * VDIM] = jnp.dot(
            latent_out,
            value_up[:, h * VDIM : (h + 1) * VDIM],
            preferred_element_type=jnp.float32,
        ).astype(jnp.bfloat16)

    def project(k):
        columns = pl.ds(pl.multiple_of(lax.rem(head + k, n_head) * cols, cols), cols)
        return jnp.dot(head_out[...], out_proj[:, columns], preferred_element_type=jnp.float32)

    def exchange(k):
        return pltpu.make_async_remote_copy(
            src_ref=outbox.at[k],
            dst_ref=inbox.at[k],
            send_sem=zsend_sem.at[k],
            recv_sem=zrecv_sem.at[k],
            device_id=head_dev(k),
            device_id_type=MESH,
        )

    for k in range(1, n_head):
        outbox[k] = project(k).astype(jnp.bfloat16)
        exchange(k).start()
    mixed = project(0)
    for k in range(1, n_head):
        exchange(k).wait_recv()
        mixed = mixed + inbox[k].astype(jnp.float32)
    mixed_ref[...] = mixed.astype(mixed_ref.dtype)

    for k in range(1, n_head):
        exchange(k).wait_send()

    def drain(copies):
        for copy in copies:
            copy.wait_send()

    loop(1, chips, lambda r: drain(sends(r)))
    loop(0, chips, lambda r: drain(forwards(r)))


def shards(sizes, query_nope, query_rope, cache, span_ids, key_up, value_up, out_proj):
    n_head, n_outer, n_inner = sizes
    chips = n_outer // CORES * n_inner
    rows = cache.shape[0]
    heads = key_up.shape[1] // NOPE
    cols = out_proj.shape[1] // n_head
    offsets = jnp.arange(SPAN, dtype=jnp.int32)
    position = (span_ids[:, None] * SPAN + offsets[None, :]).reshape(rows)
    kpos = jnp.broadcast_to(position[None, :], (8, rows))
    qpos = jnp.broadcast_to(position[:, None], (rows, 128))
    anywhere = pl.BlockSpec(memory_space=pl.ANY)
    return pl.pallas_call(
        functools.partial(kernel, sizes),
        out_shape=jax.ShapeDtypeStruct((rows, cols), jnp.bfloat16),
        in_specs=[anywhere] * 8,
        out_specs=pl.BlockSpec(memory_space=pltpu.VMEM),
        scratch_shapes=[
            pltpu.VMEM(query_nope.shape, jnp.bfloat16),
            pltpu.VMEM(query_rope.shape, jnp.bfloat16),
            pltpu.VMEM((chips, CORES * rows, LATENT + ROPE), jnp.bfloat16),
            pltpu.VMEM((chips, CORES, 8, rows), jnp.int32),
            pltpu.VMEM((rows, 128), jnp.int32),
            pltpu.VMEM(key_up.shape, jnp.bfloat16),
            pltpu.VMEM(value_up.shape, jnp.bfloat16),
            pltpu.VMEM(out_proj.shape, jnp.bfloat16),
            pltpu.VMEM((heads * rows, LATENT + ROPE), jnp.bfloat16),
            pltpu.VMEM((heads * rows, LATENT), jnp.float32),
            pltpu.VMEM((heads * rows, 1), jnp.float32),
            pltpu.VMEM((heads * rows, 1), jnp.float32),
            pltpu.VMEM((rows, heads * VDIM), jnp.bfloat16),
            pltpu.VMEM((n_head, rows, cols), jnp.bfloat16),
            pltpu.VMEM((n_head, rows, cols), jnp.bfloat16),
            pltpu.SemaphoreType.DMA((8,)),
            pltpu.SemaphoreType.DMA((2, chips)),
            pltpu.SemaphoreType.DMA((2, chips)),
            pltpu.SemaphoreType.DMA((2, chips)),
            pltpu.SemaphoreType.DMA((2, chips)),
            pltpu.SemaphoreType.DMA((n_head,)),
            pltpu.SemaphoreType.DMA((n_head,)),
        ],
        compiler_params=pltpu.CompilerParams(
            collective_id=0, has_side_effects=True, vmem_limit_bytes=60000 * 1024
        ),
    )(query_nope, query_rope, cache, kpos, qpos, key_up, value_up, out_proj)


def solution(mesh):
    sizes = (mesh.shape["head"], mesh.shape["outer"], mesh.shape["inner"])
    return jax.shard_map(
        functools.partial(shards, sizes),
        mesh=mesh,
        in_specs=(
            P(("outer", "inner"), "head"),
            P(("outer", "inner"), "head"),
            P(("outer", "inner"), None),
            P(("outer", "inner")),
            P(None, "head"),
            P(None, "head"),
            P("head", None),
        ),
        out_specs=P(("outer", "inner"), "head"),
        check_vma=False,
    )
```

```python
import functools
import math

import jax
import jax.numpy as jnp
from jax import lax
from jax.experimental import pallas as pl
from jax.experimental.pallas import tpu as pltpu
from jax.sharding import PartitionSpec as P

LATENT = 512
ROPE = 64
NOPE = 128
VDIM = 128
SPAN = 64
CORES = 2
PIECES = 4
MESH = pl.DeviceIdType.MESH


def loop(start, stop, body):
    if stop - start <= 4:
        for step in range(start, stop):
            body(step)
    else:
        lax.fori_loop(start, stop, lambda step, carry: (body(step), carry)[1], 0)


def kernel(
    sizes,
    span_ref,
    nope_hbm,
    rope_hbm,
    cache_hbm,
    key_up_hbm,
    value_up_hbm,
    out_proj_hbm,
    mixed_ref,
    nope,
    rope,
    kv,
    kpos,
    key_up,
    value_up,
    out_proj,
    queries,
    acc,
    top,
    total,
    head_out,
    outbox,
    inbox,
    halfway,
    local_sem,
    send_sem,
    recv_sem,
    fsend_sem,
    frecv_sem,
    zsend_sem,
    zrecv_sem,
    hrecv_sem,
):
    n_head, n_outer, n_inner = sizes
    chip_rows = n_outer // CORES
    chips = chip_rows * n_inner
    square = chip_rows == 2 and n_inner == 2
    width, rows = cache_hbm.shape
    heads = key_up_hbm.shape[1] // NOPE
    cols = mixed_ref.shape[1]
    piece = cols // PIECES
    head = lax.axis_index("head")
    outer = lax.axis_index("outer")
    inner = lax.axis_index("inner")
    core = lax.rem(outer, CORES)
    chip_row = outer // CORES
    peer = {"outer": chip_row * CORES + 1 - core}

    def chip(r):
        to_row = lax.rem(chip_row + r // n_inner, chip_rows)
        to_col = lax.rem(inner + r % n_inner, n_inner)
        return {"outer": to_row * CORES + core, "inner": to_col}

    loads = [
        pltpu.make_async_copy(src, dst, local_sem.at[slot])
        for slot, (src, dst) in enumerate(
            (
                (cache_hbm, kv.at[0, 0]),
                (nope_hbm, nope),
                (key_up_hbm, key_up),
                (rope_hbm, rope),
                (value_up_hbm, value_up),
                (out_proj_hbm, out_proj),
            )
        )
    ]
    for load in loads:
        load.start()

    def positions(shape, axis):
        index = lax.broadcasted_iota(jnp.int32, shape, axis)
        place = index
        for span in range(rows // SPAN):
            inside = (index >= span * SPAN) & (index < (span + 1) * SPAN)
            place = jnp.where(inside, span_ref[span] * SPAN + (index - span * SPAN), place)
        return place

    kpos[0, 0] = positions((8, rows), 1)

    barrier = pltpu.get_barrier_semaphore()
    pl.semaphore_signal(barrier, inc=1, device_id=peer, device_id_type=MESH)
    loop(
        1,
        chips,
        lambda r: pl.semaphore_signal(barrier, inc=1, device_id=chip(r), device_id_type=MESH),
    )
    for k in range(1, n_head):
        pl.semaphore_signal(
            barrier, inc=1, device_id={"head": lax.rem(head + k, n_head)}, device_id_type=MESH
        )
    pl.semaphore_wait(barrier, 1 + (chips - 1) + (n_head - 1))

    def remote(src, dst, send, recv, device):
        return pltpu.make_async_remote_copy(
            src_ref=src,
            dst_ref=dst,
            send_sem=send,
            recv_sem=recv,
            device_id=device,
            device_id_type=MESH,
        )

    def send_positions(r):
        return remote(
            kpos.at[0, 0], kpos.at[r, 0], send_sem.at[2, r], recv_sem.at[2, r], chip(r)
        )

    def send_block(r):
        return remote(kv.at[0, 0], kv.at[r, 0], send_sem.at[0, r], recv_sem.at[0, r], chip(r))

    def send_half(source, slot, p, to):
        part = pl.ds(p * (width // 2), width // 2)
        return remote(
            kv.at[source, 0, part],
            kv.at[slot, 0, part],
            send_sem.at[p, slot],
            recv_sem.at[p, slot],
            chip(to),
        )

    def forwards(r):
        return (
            remote(kv.at[r, 0], kv.at[r, 1], fsend_sem.at[0, r], frecv_sem.at[0, r], peer),
            remote(kpos.at[r, 0], kpos.at[r, 1], fsend_sem.at[1, r], frecv_sem.at[1, r], peer),
        )

    def forward(r):
        send_positions(r).wait_recv()
        for copy in forwards(r):
            copy.start()

    loads[0].wait()
    if square:
        for p in range(2):
            send_half(0, 2, p, 2).start()
            send_half(0, 1, 1 - p, 1).start()
    else:
        loop(1, chips, lambda r: send_block(r).start())
    for copy in forwards(0):
        copy.start()
    loop(1, chips, lambda r: send_positions(r).start())

    loads[1].wait()
    loads[2].wait()
    loads[3].wait()
    for h in range(heads):
        block = slice(h * NOPE, (h + 1) * NOPE)
        q_latent = lax.dot_general(
            nope[:, block],
            key_up[:, block],
            (((1,), (1,)), ((), ())),
            preferred_element_type=jnp.float32,
        )
        queries[h * rows : (h + 1) * rows, :LATENT] = q_latent.astype(jnp.bfloat16)
        queries[h * rows : (h + 1) * rows, LATENT:] = rope[:, h * ROPE : (h + 1) * ROPE]

    scale = (NOPE + ROPE) ** (-0.5) * math.log2(math.e)

    def attend(r, first):
        for copy in forwards(r):
            copy.wait_recv()
        keys = jnp.concatenate([kv[r, 0], kv[r, 1]], axis=1)
        scores = jnp.dot(queries[...], keys, preferred_element_type=jnp.float32) * scale
        at_key = jnp.concatenate([kpos[r, 0][:1], kpos[r, 1][:1]], axis=1)
        at_query = positions((rows, CORES * rows), 0)
        visible = at_key <= at_query
        scores = jnp.where(
            visible[None], scores.reshape(heads, rows, CORES * rows), -jnp.inf
        ).reshape(heads * rows, CORES * rows)
        high = jnp.max(scores, axis=1, keepdims=True)
        if not first:
            before = top[...]
            high = jnp.maximum(before, high)
            rescale = jnp.exp2(before - high)
        weights = jnp.exp2(scores - high)
        added = jnp.sum(weights, axis=1, keepdims=True)
        part = lax.dot_general(
            weights.astype(jnp.bfloat16),
            keys[:LATENT],
            (((1,), (1,)), ((), ())),
            preferred_element_type=jnp.float32,
        )
        top[...] = high
        if first:
            total[...] = added
            acc[...] = part
        else:
            total[...] = total[...] * rescale + added
            acc[...] = acc[...] * rescale + part

    attend(0, True)
    if square:
        send_half(0, 2, 0, 2).wait_recv()
        send_half(2, 3, 0, 1).start()
        send_half(0, 1, 1, 1).wait_recv()
        send_half(1, 3, 1, 2).start()
        send_half(0, 2, 1, 2).wait_recv()
        forward(2)
        send_half(0, 1, 0, 1).wait_recv()
        forward(1)
        attend(2, False)
        attend(1, False)
        send_half(2, 3, 0, 1).wait_recv()
        send_half(1, 3, 1, 2).wait_recv()
        forward(3)
        attend(3, False)
    else:

        def relay(r):
            send_block(r).wait_recv()
            forward(r)

        loop(1, chips, relay)
        loop(1, chips, lambda r: attend(r, False))

    loads[4].wait()
    loads[5].wait()
    for h in range(heads):
        block = slice(h * rows, (h + 1) * rows)
        latent_out = (acc[block] / total[block]).astype(jnp.bfloat16)
        head_out[:, h * VDIM : (h + 1) * VDIM] = jnp.dot(
            latent_out,
            value_up[:, h * VDIM : (h + 1) * VDIM],
            preferred_element_type=jnp.float32,
        ).astype(jnp.bfloat16)

    def project(d):
        return jnp.dot(
            head_out[...], out_proj[:, d * cols : (d + 1) * cols], preferred_element_type=jnp.float32
        )

    last = n_head - 1

    def stop(z, d):
        if z == 0 and d >= 2:
            return 1
        if z == last and d <= last - 2:
            return last - 1
        return d

    def exchange(z, d, q):
        via = stop(z, d)
        if via == d:
            dst, recv = inbox.at[z, q], zrecv_sem.at[z, q]
        else:
            dst, recv = halfway.at[d, q], hrecv_sem.at[d, q]
        return remote(outbox.at[d, q], dst, zsend_sem.at[d, q], recv, {"head": via})

    def through(z, d):
        return [s for s in range(n_head) if s != z and s != d and stop(s, d) == z]

    def finish(z):
        far = sorted((d for d in range(n_head) if d != z), key=lambda d: -abs(d - z))
        own = [d for d in far if not through(z, d)]
        joined = [d for d in far if through(z, d)]
        for d in own + joined:
            part = project(d)
            for q in range(PIECES):
                sent = part[:, q * piece : (q + 1) * piece]
                for s in through(z, d):
                    exchange(s, d, q).wait_recv()
                    sent = sent + halfway[d, q].astype(jnp.float32)
                outbox[d, q] = sent.astype(jnp.bfloat16)
                exchange(z, d, q).start()
        mixed = project(z)
        sources = [s for s in range(n_head) if s != z and stop(s, z) == z]
        for q in range(PIECES):
            part = mixed[:, q * piece : (q + 1) * piece]
            for s in sources:
                exchange(s, z, q).wait_recv()
                part = part + inbox[s, q].astype(jnp.float32)
            mixed_ref[:, q * piece : (q + 1) * piece] = part.astype(mixed_ref.dtype)
        for d in far:
            for q in range(PIECES):
                exchange(z, d, q).wait_send()

    for z in range(n_head):
        pl.when(head == z)(functools.partial(finish, z))

    if square:
        for p in range(2):
            send_half(0, 2, p, 2).wait_send()
            send_half(0, 1, 1 - p, 1).wait_send()
        send_half(2, 3, 0, 1).wait_send()
        send_half(1, 3, 1, 2).wait_send()
    else:
        loop(1, chips, lambda r: send_block(r).wait_send())
    loop(1, chips, lambda r: send_positions(r).wait_send())

    def drain(r):
        for copy in forwards(r):
            copy.wait_send()

    loop(0, chips, drain)


def shards(sizes, query_nope, query_rope, cache, span_ids, key_up, value_up, out_proj):
    n_head, n_outer, n_inner = sizes
    chips = n_outer // CORES * n_inner
    rows = cache.shape[0]
    heads = key_up.shape[1] // NOPE
    cols = out_proj.shape[1] // n_head
    anywhere = pl.BlockSpec(memory_space=pl.ANY)
    boxes = pltpu.VMEM((n_head, PIECES, rows, cols // PIECES), jnp.bfloat16)
    return pl.pallas_call(
        functools.partial(kernel, sizes),
        out_shape=jax.ShapeDtypeStruct((rows, cols), jnp.bfloat16),
        in_specs=[pl.BlockSpec(memory_space=pltpu.SMEM)] + [anywhere] * 6,
        out_specs=pl.BlockSpec(memory_space=pltpu.VMEM),
        scratch_shapes=[
            pltpu.VMEM(query_nope.shape, jnp.bfloat16),
            pltpu.VMEM(query_rope.shape, jnp.bfloat16),
            pltpu.VMEM((chips, CORES, LATENT + ROPE, rows), jnp.bfloat16),
            pltpu.VMEM((chips, CORES, 8, rows), jnp.int32),
            pltpu.VMEM(key_up.shape, jnp.bfloat16),
            pltpu.VMEM(value_up.shape, jnp.bfloat16),
            pltpu.VMEM(out_proj.shape, jnp.bfloat16),
            pltpu.VMEM((heads * rows, LATENT + ROPE), jnp.bfloat16),
            pltpu.VMEM((heads * rows, LATENT), jnp.float32),
            pltpu.VMEM((heads * rows, 1), jnp.float32),
            pltpu.VMEM((heads * rows, 1), jnp.float32),
            pltpu.VMEM((rows, heads * VDIM), jnp.bfloat16),
            boxes,
            boxes,
            boxes,
            pltpu.SemaphoreType.DMA((6,)),
            pltpu.SemaphoreType.DMA((3, chips)),
            pltpu.SemaphoreType.DMA((3, chips)),
            pltpu.SemaphoreType.DMA((2, chips)),
            pltpu.SemaphoreType.DMA((2, chips)),
            pltpu.SemaphoreType.DMA((n_head, PIECES)),
            pltpu.SemaphoreType.DMA((n_head, PIECES)),
            pltpu.SemaphoreType.DMA((n_head, PIECES)),
        ],
        compiler_params=pltpu.CompilerParams(
            collective_id=0, has_side_effects=True, vmem_limit_bytes=60000 * 1024
        ),
    )(span_ids, query_nope, query_rope, cache.T, key_up, value_up, out_proj)


def solution(mesh):
    sizes = (mesh.shape["head"], mesh.shape["outer"], mesh.shape["inner"])
    return jax.shard_map(
        functools.partial(shards, sizes),
        mesh=mesh,
        in_specs=(
            P(("outer", "inner"), "head"),
            P(("outer", "inner"), "head"),
            P(("outer", "inner"), None),
            P(("outer", "inner")),
            P(None, "head"),
            P(None, "head"),
            P("head", None),
        ),
        out_specs=P(("outer", "inner"), "head"),
        check_vma=False,
    )
```

```python
import functools
import math

import jax
import jax.numpy as jnp
from jax import lax
from jax.experimental import pallas as pl
from jax.experimental.pallas import tpu as pltpu
from jax.sharding import PartitionSpec as P

LATENT = 512
ROPE = 64
NOPE = 128
VDIM = 128
SPAN = 64
CORES = 2
PIECES = 4
MESH = pl.DeviceIdType.MESH


def loop(start, stop, body):
    if stop - start <= 4:
        for step in range(start, stop):
            body(step)
    else:
        lax.fori_loop(start, stop, lambda step, carry: (body(step), carry)[1], 0)


def kernel(
    sizes,
    span_hbm,
    nope_hbm,
    rope_hbm,
    cache_hbm,
    key_up_hbm,
    value_up_hbm,
    out_proj_hbm,
    mixed_ref,
    nope,
    rope,
    kv,
    kpos,
    span_ref,
    key_up,
    value_up,
    out_proj,
    queries,
    acc,
    top,
    total,
    head_out,
    outbox,
    inbox,
    halfway,
    local_sem,
    send_sem,
    recv_sem,
    fsend_sem,
    frecv_sem,
    zsend_sem,
    zrecv_sem,
    hrecv_sem,
):
    n_head, n_outer, n_inner = sizes
    chip_rows = n_outer // CORES
    chips = chip_rows * n_inner
    square = chip_rows == 2 and n_inner == 2
    width, rows = cache_hbm.shape
    heads = key_up_hbm.shape[1] // NOPE
    cols = mixed_ref.shape[1]
    piece = cols // 2
    half_rows = rows // 2
    group = heads * half_rows
    head = lax.axis_index("head")
    outer = lax.axis_index("outer")
    inner = lax.axis_index("inner")
    core = lax.rem(outer, CORES)
    chip_row = outer // CORES
    peer = {"outer": chip_row * CORES + 1 - core}

    def chip(r):
        to_row = lax.rem(chip_row + r // n_inner, chip_rows)
        to_col = lax.rem(inner + r % n_inner, n_inner)
        return {"outer": to_row * CORES + core, "inner": to_col}

    loads = [
        pltpu.make_async_copy(src, dst, local_sem.at[slot])
        for slot, (src, dst) in enumerate(
            (
                (cache_hbm, kv.at[0, 0]),
                (nope_hbm, nope),
                (key_up_hbm, key_up),
                (rope_hbm, rope),
                (value_up_hbm, value_up),
                (out_proj_hbm, out_proj),
                (span_hbm, span_ref),
            )
        )
    ]
    loads[6].start()
    for load in loads[:6]:
        load.start()

    def positions(shape, axis):
        index = lax.broadcasted_iota(jnp.int32, shape, axis)
        place = index
        for span in range(rows // SPAN):
            inside = (index >= span * SPAN) & (index < (span + 1) * SPAN)
            place = jnp.where(inside, span_ref[span] * SPAN + (index - span * SPAN), place)
        return place

    barrier = pltpu.get_barrier_semaphore()
    pl.semaphore_signal(barrier, inc=1, device_id=peer, device_id_type=MESH)
    loop(
        1,
        chips,
        lambda r: pl.semaphore_signal(barrier, inc=1, device_id=chip(r), device_id_type=MESH),
    )
    for k in range(1, n_head):
        pl.semaphore_signal(
            barrier, inc=1, device_id={"head": lax.rem(head + k, n_head)}, device_id_type=MESH
        )
    pl.semaphore_wait(barrier, 1 + (chips - 1) + (n_head - 1))

    def remote(src, dst, send, recv, device):
        return pltpu.make_async_remote_copy(
            src_ref=src,
            dst_ref=dst,
            send_sem=send,
            recv_sem=recv,
            device_id=device,
            device_id_type=MESH,
        )

    def send_positions(r):
        return remote(
            kpos.at[0, 0], kpos.at[r, 0], send_sem.at[2, r], recv_sem.at[2, r], chip(r)
        )

    def send_block(r):
        return remote(kv.at[0, 0], kv.at[r, 0], send_sem.at[0, r], recv_sem.at[0, r], chip(r))

    def send_half(source, slot, p, to):
        part = pl.ds(p * (width // 2), width // 2)
        return remote(
            kv.at[source, 0, part],
            kv.at[slot, 0, part],
            send_sem.at[p, slot],
            recv_sem.at[p, slot],
            chip(to),
        )

    def forwards(r):
        return (
            remote(kv.at[r, 0], kv.at[r, 1], fsend_sem.at[0, r], frecv_sem.at[0, r], peer),
            remote(kpos.at[r, 0], kpos.at[r, 1], fsend_sem.at[1, r], frecv_sem.at[1, r], peer),
        )

    def forward(r):
        send_positions(r).wait_recv()
        for copy in forwards(r):
            copy.start()

    loads[6].wait()
    kpos[0, 0] = positions((8, rows), 1)
    loads[0].wait()
    if square:
        for p in range(2):
            send_half(0, 2, p, 2).start()
            send_half(0, 1, 1 - p, 1).start()
    else:
        loop(1, chips, lambda r: send_block(r).start())
    for copy in forwards(0):
        copy.start()
    loop(1, chips, lambda r: send_positions(r).start())

    loads[1].wait()
    loads[2].wait()
    loads[3].wait()
    for h in range(heads):
        block = slice(h * NOPE, (h + 1) * NOPE)
        q_latent = lax.dot_general(
            nope[:, block],
            key_up[:, block],
            (((1,), (1,)), ((), ())),
            preferred_element_type=jnp.float32,
        )
        for half in range(2):
            place = slice(half * group + h * half_rows, half * group + (h + 1) * half_rows)
            taken = slice(half * half_rows, (half + 1) * half_rows)
            queries[place, :LATENT] = q_latent[taken].astype(jnp.bfloat16)
            queries[place, LATENT:] = rope[taken, h * ROPE : (h + 1) * ROPE]

    scale = (NOPE + ROPE) ** (-0.5) * math.log2(math.e)

    def arrive(r):
        for copy in forwards(r):
            copy.wait_recv()

    def attend(r, first, halves=(0, 1)):
        mine = slice(halves[0] * group, (halves[-1] + 1) * group)
        keys = jnp.concatenate([kv[r, 0], kv[r, 1]], axis=1)
        scores = jnp.dot(queries[mine], keys, preferred_element_type=jnp.float32) * scale
        at_key = jnp.concatenate([kpos[r, 0][:1], kpos[r, 1][:1]], axis=1)
        at_query = positions((rows, CORES * rows), 0)
        at_query = at_query[halves[0] * half_rows : (halves[-1] + 1) * half_rows]
        visible = (at_key <= at_query).reshape(len(halves), 1, half_rows, CORES * rows)
        scores = jnp.where(
            visible, scores.reshape(len(halves), heads, half_rows, CORES * rows), -jnp.inf
        ).reshape(len(halves) * group, CORES * rows)
        high = jnp.max(scores, axis=1, keepdims=True)
        if not first:
            before = top[mine]
            high = jnp.maximum(before, high)
            rescale = jnp.exp2(before - high)
        weights = jnp.exp2(scores - high)
        added = jnp.sum(weights, axis=1, keepdims=True)
        part = lax.dot_general(
            weights.astype(jnp.bfloat16),
            keys[:LATENT],
            (((1,), (1,)), ((), ())),
            preferred_element_type=jnp.float32,
        )
        top[mine] = high
        if first:
            total[mine] = added
            acc[mine] = part
        else:
            total[mine] = total[mine] * rescale + added
            acc[mine] = acc[mine] * rescale + part

    arrive(0)
    attend(0, True)
    if square:
        send_half(0, 2, 0, 2).wait_recv()
        send_half(2, 3, 0, 1).start()
        send_half(0, 1, 1, 1).wait_recv()
        send_half(1, 3, 1, 2).start()
        send_half(0, 2, 1, 2).wait_recv()
        forward(2)
        send_half(0, 1, 0, 1).wait_recv()
        forward(1)
        arrive(2)
        attend(2, False)
        send_half(2, 3, 0, 1).wait_recv()
        send_half(1, 3, 1, 2).wait_recv()
        forward(3)
        arrive(1)
        attend(1, False)
    else:

        def relay(r):
            send_block(r).wait_recv()
            forward(r)

        loop(1, chips, relay)
        loop(1, chips, arrive)
        loop(1, chips - 1, lambda r: attend(r, False))

    if square:
        arrive(3)
    loads[4].wait()
    loads[5].wait()

    def close(half):
        attend(chips - 1, False, (half,))
        for h in range(heads):
            block = slice(half * group + h * half_rows, half * group + (h + 1) * half_rows)
            latent_out = (acc[block] / total[block]).astype(jnp.bfloat16)
            head_out[half * half_rows : (half + 1) * half_rows, h * VDIM : (h + 1) * VDIM] = (
                jnp.dot(
                    latent_out,
                    value_up[:, h * VDIM : (h + 1) * VDIM],
                    preferred_element_type=jnp.float32,
                ).astype(jnp.bfloat16)
            )

    def project(d, half):
        return jnp.dot(
            head_out[half * half_rows : (half + 1) * half_rows],
            out_proj[:, d * cols : (d + 1) * cols],
            preferred_element_type=jnp.float32,
        )

    last = n_head - 1

    def stop(z, d):
        if z == 0 and d >= 2:
            return 1
        if z == last and d <= last - 2:
            return last - 1
        return d

    def exchange(z, d, q):
        via = stop(z, d)
        if via == d:
            dst, recv = inbox.at[z, q], zrecv_sem.at[z, q]
        else:
            dst, recv = halfway.at[d, q], hrecv_sem.at[d, q]
        return remote(outbox.at[d, q], dst, zsend_sem.at[d, q], recv, {"head": via})

    def through(z, d):
        return [s for s in range(n_head) if s != z and s != d and stop(s, d) == z]

    def plan(z):
        far = sorted((d for d in range(n_head) if d != z), key=lambda d: -abs(d - z))
        own = [d for d in far if not through(z, d)]
        early = [d for d in own if stop(z, d) != d] or own
        late = [d for d in far if d not in early]
        return early, late

    def give(z, d, half):
        part = project(d, half)
        for c in range(2):
            q = 2 * half + c
            sent = part[:, c * piece : (c + 1) * piece]
            for s in through(z, d):
                exchange(s, d, q).wait_recv()
                sent = sent + halfway[d, q].astype(jnp.float32)
            outbox[d, q] = sent.astype(jnp.bfloat16)
            exchange(z, d, q).start()

    def begin(z, half):
        for d in plan(z)[0]:
            give(z, d, half)

    def finish(z):
        early, late = plan(z)
        for d in late:
            for half in range(2):
                give(z, d, half)
        sources = [s for s in range(n_head) if s != z and stop(s, z) == z]
        for half in range(2):
            mixed = project(z, half)
            for c in range(2):
                part = mixed[:, c * piece : (c + 1) * piece]
                for s in sources:
                    exchange(s, z, 2 * half + c).wait_recv()
                    part = part + inbox[s, 2 * half + c].astype(jnp.float32)
                mixed_ref[
                    half * half_rows : (half + 1) * half_rows, c * piece : (c + 1) * piece
                ] = part.astype(mixed_ref.dtype)
        for d in early + late:
            for q in range(PIECES):
                exchange(z, d, q).wait_send()

    for half in range(2):
        close(half)
        for z in range(n_head):
            pl.when(head == z)(functools.partial(begin, z, half))
    for z in range(n_head):
        pl.when(head == z)(functools.partial(finish, z))

    if square:
        for p in range(2):
            send_half(0, 2, p, 2).wait_send()
            send_half(0, 1, 1 - p, 1).wait_send()
        send_half(2, 3, 0, 1).wait_send()
        send_half(1, 3, 1, 2).wait_send()
    else:
        loop(1, chips, lambda r: send_block(r).wait_send())
    loop(1, chips, lambda r: send_positions(r).wait_send())

    def drain(r):
        for copy in forwards(r):
            copy.wait_send()

    loop(0, chips, drain)


def shards(sizes, query_nope, query_rope, cache, span_ids, key_up, value_up, out_proj):
    n_head, n_outer, n_inner = sizes
    chips = n_outer // CORES * n_inner
    rows = cache.shape[0]
    heads = key_up.shape[1] // NOPE
    cols = out_proj.shape[1] // n_head
    anywhere = pl.BlockSpec(memory_space=pl.ANY)
    boxes = pltpu.VMEM((n_head, PIECES, rows // 2, cols // 2), jnp.bfloat16)
    return pl.pallas_call(
        functools.partial(kernel, sizes),
        out_shape=jax.ShapeDtypeStruct((rows, cols), jnp.bfloat16),
        in_specs=[anywhere] * 7,
        out_specs=pl.BlockSpec(memory_space=pltpu.VMEM),
        scratch_shapes=[
            pltpu.VMEM(query_nope.shape, jnp.bfloat16),
            pltpu.VMEM(query_rope.shape, jnp.bfloat16),
            pltpu.VMEM((chips, CORES, LATENT + ROPE, rows), jnp.bfloat16),
            pltpu.VMEM((chips, CORES, 8, rows), jnp.int32),
            pltpu.SMEM(span_ids.shape, jnp.int32),
            pltpu.VMEM(key_up.shape, jnp.bfloat16),
            pltpu.VMEM(value_up.shape, jnp.bfloat16),
            pltpu.VMEM(out_proj.shape, jnp.bfloat16),
            pltpu.VMEM((heads * rows, LATENT + ROPE), jnp.bfloat16),
            pltpu.VMEM((heads * rows, LATENT), jnp.float32),
            pltpu.VMEM((heads * rows, 1), jnp.float32),
            pltpu.VMEM((heads * rows, 1), jnp.float32),
            pltpu.VMEM((rows, heads * VDIM), jnp.bfloat16),
            boxes,
            boxes,
            boxes,
            pltpu.SemaphoreType.DMA((7,)),
            pltpu.SemaphoreType.DMA((3, chips)),
            pltpu.SemaphoreType.DMA((3, chips)),
            pltpu.SemaphoreType.DMA((2, chips)),
            pltpu.SemaphoreType.DMA((2, chips)),
            pltpu.SemaphoreType.DMA((n_head, PIECES)),
            pltpu.SemaphoreType.DMA((n_head, PIECES)),
            pltpu.SemaphoreType.DMA((n_head, PIECES)),
        ],
        compiler_params=pltpu.CompilerParams(
            collective_id=0, has_side_effects=True, vmem_limit_bytes=60000 * 1024
        ),
    )(span_ids, query_nope, query_rope, cache.T, key_up, value_up, out_proj)


def solution(mesh):
    sizes = (mesh.shape["head"], mesh.shape["outer"], mesh.shape["inner"])
    return jax.shard_map(
        functools.partial(shards, sizes),
        mesh=mesh,
        in_specs=(
            P(("outer", "inner"), "head"),
            P(("outer", "inner"), "head"),
            P(("outer", "inner"), None),
            P(("outer", "inner")),
            P(None, "head"),
            P(None, "head"),
            P("head", None),
        ),
        out_specs=P(("outer", "inner"), "head"),
        check_vma=False,
    )
```
